32 devices in a mesh: seq: 16 (over z, y, x), head: 2 (over core).
Axes of the slice: x: 2, y: 2, z: 4, core: 2. Of those that a mesh axis runs over, the one named last changes fastest.
Arguments:
- acceptance_signal: bfloat16 [8192, 2048], P(('seq', 'head')), may hold values from -6 to 6
- lookup_entries: bfloat16 [8192, 2048], P(('seq', 'head')), may hold values from -6 to 6
- content_entries: bfloat16 [8192, 2048], P(('seq', 'head')), may hold values from -6 to 6
- fading_exponent_table: bfloat16 [8192, 2048], P(('seq', 'head')), may hold values from -17 to 0
- raw_control_signal: bfloat16 [8192, 2048], P(('seq', 'head')), may hold values from -6 to 6
- current_token_reward: float32 [32, 64], P('head'), may hold values from -1 to 1
- slice_scaling_factor: float32 [2048], P('head'), may hold values from 0.1 to 1.9
- result_mapping: bfloat16 [2048, 4096], P('head'), may hold values from -0.125 to 0.125
Outputs:
- time_mixed: bfloat16 [8192, 4096], P(('seq', 'head'))
The draws below stay inside these ranges and needn't reach their ends.
All inputs are finite; a program needn't handle non-finite values.
Results may differ from the reference program's by a relative error of at most 0.009.
Values may be sent and summed in bfloat16 or wider, within the bound.
A program may use at most 192 MiB of HBM per device.

```python
import math
import jax
import jax.numpy as jnp
from jax import lax

D = 4096
ATTENTION_SLICES = 32
SLICE_BREADTH = 64
BLOCK = 128
TOK_SEQ = 512
TOKEN_SPAN = 8192


def draw_fading_exponent_table(key, part):
    hidden_breadth = ATTENTION_SLICES * SLICE_BREADTH
    lookup_lines = jax.random.split(jax.random.fold_in(key, 7), 7)
    share = 0.5
    fast_heads = jax.random.uniform(lookup_lines[0], (ATTENTION_SLICES,)) < share
    fast_rate = jnp.exp(jax.random.uniform(lookup_lines[1], (ATTENTION_SLICES, SLICE_BREADTH), jnp.float32, math.log(1.0 / 50.0), math.log(1.0 / 30.0)))
    slow_rate = jnp.exp(jax.random.uniform(lookup_lines[2], (ATTENTION_SLICES, SLICE_BREADTH), jnp.float32, math.log(1.0 / (8.0 * TOK_SEQ)), math.log(1.0 / TOK_SEQ)))
    base = jnp.where(fast_heads[:, None], fast_rate, slow_rate).reshape(hidden_breadth)
    token_factor = jnp.exp(jax.random.uniform(lookup_lines[3], (TOKEN_SPAN, hidden_breadth), jnp.float32, -math.log(2.0), math.log(2.0)))
    groups = TOKEN_SPAN // TOK_SEQ
    group_factor = jnp.exp(jax.random.uniform(lookup_lines[4], (groups, 1, hidden_breadth), jnp.float32, -math.log(2.0), math.log(2.0)))
    fading_quickness = (token_factor.reshape(groups, TOK_SEQ, hidden_breadth) * group_factor).reshape(TOKEN_SPAN, hidden_breadth) * base[None]
    spike_location = jax.random.randint(lookup_lines[5], (3,), 0, TOKEN_SPAN)
    spike_portion = jax.random.uniform(lookup_lines[6], (3, hidden_breadth), jnp.float32, 0.2, 0.5)
    spike_quickness = -jnp.log(1.0 - spike_portion)
    indicator_selector = (jnp.arange(TOKEN_SPAN)[:, None] == spike_location[None, :]).astype(jnp.float32)
    fading_quickness = fading_quickness + jnp.dot(indicator_selector, spike_quickness)
    return jnp.log(fading_quickness).astype(jnp.bfloat16)


def level_of(key, shape, cuts, least, high):
    level, own = 1.0, jax.random.fold_in(key, 6)
    for axis_at, shards_of in cuts:
        heights = jnp.exp(jax.random.uniform(jax.random.fold_in(own, axis_at), (shards_of,), jnp.float32, least / len(cuts), high / len(cuts)))
        level = level * jnp.repeat(heights, shape[axis_at] // shards_of).reshape([-1 if axis == axis_at else 1 for axis in range(len(shape))])
    return level


def normal_values(own_key, dims, width, most, cuts=(), dtype=jnp.bfloat16):
    loudness = level_of(own_key, dims, cuts, -0.22, 0.18) if cuts else 1.0
    drawn = jax.random.normal(own_key, dims, jnp.float32) * width * loudness
    return jnp.minimum(jnp.maximum(drawn, -most), most).astype(dtype)


def setup_inputs(seed: int = 0) -> dict:
    key_of = jax.random.split(jax.random.key(seed), 9)
    acceptance_signal = normal_values(key_of[0], (TOKEN_SPAN, ATTENTION_SLICES * SLICE_BREADTH), 1.0, 6.0, ((0, 32),))
    lookup_entries = normal_values(key_of[1], (TOKEN_SPAN, ATTENTION_SLICES * SLICE_BREADTH), 1.0, 6.0, ((0, 32),))
    content_entries = normal_values(key_of[2], (TOKEN_SPAN, ATTENTION_SLICES * SLICE_BREADTH), 1.0, 6.0, ((0, 32),))
    fading_exponent_table = draw_fading_exponent_table(jax.random.fold_in(key_of[8], 71), 0)
    raw_control_signal = normal_values(key_of[4], (TOKEN_SPAN, ATTENTION_SLICES * SLICE_BREADTH), 1.0, 6.0, ((0, 32),))
    current_token_reward = jnp.clip(jax.random.uniform(key_of[5], (ATTENTION_SLICES, SLICE_BREADTH), jnp.float32, -1.0, 1.0) * level_of(key_of[5], (ATTENTION_SLICES, SLICE_BREADTH), ((0, 2),), -0.4, 0.0), -1.0, 1.0)
    slice_scaling_factor = jnp.clip(1.0 + 0.18 * jax.random.normal(key_of[6], (ATTENTION_SLICES * SLICE_BREADTH,), jnp.float32), 0.1, 1.9)
    result_mapping = normal_values(key_of[7], (ATTENTION_SLICES * SLICE_BREADTH, D), (ATTENTION_SLICES * SLICE_BREADTH) ** -0.5, 0.125, ((0, 2),))
    return {"acceptance_signal": acceptance_signal, "lookup_entries": lookup_entries, "content_entries": content_entries, "fading_exponent_table": fading_exponent_table, "raw_control_signal": raw_control_signal, "current_token_reward": current_token_reward, "slice_scaling_factor": slice_scaling_factor, "result_mapping": result_mapping}


EPS = 1e-05

def reference(acceptance_signal, lookup_entries, content_entries, fading_exponent_table, raw_control_signal, current_token_reward, slice_scaling_factor, result_mapping):
    length = acceptance_signal.shape[0]
    blocks = length // BLOCK
    high = lax.Precision.HIGHEST
    hidden_breadth = ATTENTION_SLICES * SLICE_BREADTH
    positions = jnp.arange(BLOCK)
    strict = (positions[:, None] > positions[None, :]).astype(jnp.float32)
    gain = slice_scaling_factor.reshape(ATTENTION_SLICES, SLICE_BREADTH)

    def block_step(state, inputs):
        rec_in, key_in, val_in, logit_in, gate_in = inputs
        acceptance_single_real = rec_in.astype(jnp.float32)
        lookup_single_real = key_in.astype(jnp.float32)
        content_single_real = val_in.astype(jnp.float32)
        log_decay = -jnp.exp(logit_in.astype(jnp.float32))
        cum_incl = jnp.cumsum(log_decay, axis=0)
        cum_excl = cum_incl - log_decay
        total = cum_incl[-1]
        rec_scaled = acceptance_single_real * jnp.exp(cum_excl)
        key_scaled = lookup_single_real * jnp.exp(-cum_incl)
        key_ending = lookup_single_real * jnp.exp(total[None] - cum_incl)
        scores = jnp.einsum('thi,shi->hts', rec_scaled, key_scaled, precision=high) * strict[None]
        within = jnp.einsum('hts,shj->thj', scores, content_single_real, precision=high)
        diagonal_contribution = lax.optimization_barrier(jnp.sum(acceptance_single_real * current_token_reward[None] * lookup_single_real, axis=-1, keepdims=True)) * content_single_real
        across = jnp.einsum('thi,hij->thj', rec_scaled, state, precision=high)
        output = within + diagonal_contribution + across
        new_state = jnp.exp(total)[..., None] * state + jnp.einsum('shi,shj->hij', key_ending, content_single_real, precision=high)
        mean = lax.optimization_barrier(jnp.mean(output, axis=-1, keepdims=True))
        centred = output - mean
        var = lax.optimization_barrier(jnp.mean(centred * centred, axis=-1, keepdims=True))
        normed = centred / jnp.sqrt(var + EPS) * gain[None]
        gate_f = gate_in.astype(jnp.float32)
        gated = (normed.reshape(BLOCK, hidden_breadth) * jax.nn.silu(gate_f)).astype(jnp.bfloat16)
        return (new_state, gated)
    shape4 = (blocks, BLOCK, ATTENTION_SLICES, SLICE_BREADTH)
    inputs = (acceptance_signal.reshape(shape4), lookup_entries.reshape(shape4), content_entries.reshape(shape4), fading_exponent_table.reshape(shape4), raw_control_signal.reshape(blocks, BLOCK, hidden_breadth))
    start = jnp.zeros((ATTENTION_SLICES, SLICE_BREADTH, SLICE_BREADTH), jnp.float32)
    final_state, gated = lax.scan(block_step, start, inputs)
    gated = gated.reshape(length, hidden_breadth)
    return jnp.dot(gated, result_mapping, preferred_element_type=jnp.float32).astype(jnp.bfloat16)
```

```python
import functools

import jax
import jax.numpy as jnp
from jax import lax
from jax.experimental import pallas as pl
from jax.experimental.pallas import tpu as pltpu
from jax.sharding import PartitionSpec as P

BLOCK = 128
LANES = 128
QUAD = 256
CHUNK = 512
EPS = 1e-05
MESH = pl.DeviceIdType.MESH
F32 = jnp.float32
BF16 = jnp.bfloat16


def dot(a, b):
    return jnp.dot(a, b, preferred_element_type=F32)


def dot_nt(a, b):
    return lax.dot_general(a, b, (((1,), (1,)), ((), ())), preferred_element_type=F32)


def dot_tn(a, b):
    return lax.dot_general(a, b, (((0,), (0,)), ((), ())), preferred_element_type=F32)


def split_heads(x, low):
    zero = jnp.zeros_like(x)
    return jnp.concatenate([jnp.where(low, x, zero), jnp.where(low, zero, x)], axis=0)


def kernel(
    n, breadth,
    rec_hbm, key_hbm, val_hbm, fade_hbm, gate_hbm, reward_ref, gain_ref, map_hbm,
    out_hbm,
    fade, key, val, rec, gate, weight, rec_mid, key_mid, local_out, entering, pref_row, mid_row,
    outbox, outdec, inbox, indec, outbox2, carry, gated, snd, rcv, outv,
    in_send, in_recv, in_local, w_sem, s_send, s_recv, d_send, d_recv, c_send, c_recv,
    p_send, p_recv, o_sem,
):
    me, core = lax.axis_index("seq"), lax.axis_index("head")
    other = 1 - core
    rows, width = rec_hbm.shape[0], rec.shape[1]
    tokens = rec.shape[0]
    blocks, quads, pairs = tokens // BLOCK, width // QUAD, width // LANES
    chunks = weight.shape[0]
    piece = outbox.shape[1]
    per_pair = breadth // piece
    my_rows = pl.ds(pl.multiple_of(core * rows, 128), rows)
    their_rows = pl.ds(pl.multiple_of(other * rows, 128), rows)
    my_cols = pl.ds(pl.multiple_of(core * width, 128), width)
    their_cols = pl.ds(pl.multiple_of(other * width, 128), width)
    pairs_io = ((fade_hbm, fade), (key_hbm, key), (val_hbm, val), (rec_hbm, rec), (gate_hbm, gate))

    locals_ = [
        pltpu.make_async_copy(src.at[:, my_cols], dst.at[my_rows, :], in_local.at[i])
        for i, (src, dst) in enumerate(pairs_io)
    ]
    remotes = [
        pltpu.make_async_remote_copy(
            src_ref=src.at[:, their_cols], dst_ref=dst.at[my_rows, :],
            send_sem=in_send.at[i], recv_sem=in_recv.at[i],
            device_id=(me, other), device_id_type=MESH,
        )
        for i, (src, dst) in enumerate(pairs_io)
    ]
    barrier = pltpu.get_barrier_semaphore()
    pl.semaphore_signal(barrier, inc=1, device_id=(me, other), device_id_type=MESH)

    def greet(d, c):
        pl.semaphore_signal(
            barrier, inc=1, device_id=(lax.rem(me + d, n), core), device_id_type=MESH
        )
        return c

    lax.fori_loop(1, n, greet, 0)
    for copy in locals_:
        copy.start()
    pl.semaphore_wait(barrier, n)
    for copy in remotes:
        copy.start()

    def weight_copy(c):
        return pltpu.make_async_copy(
            map_hbm.at[:, pl.ds(pl.multiple_of(c * CHUNK, CHUNK), CHUNK)], weight.at[c], w_sem.at[c]
        )

    for c in range(chunks):
        weight_copy(c).start()

    t_id = lax.broadcasted_iota(jnp.int32, (BLOCK, 2 * BLOCK), 0)
    s_id = lax.rem(lax.broadcasted_iota(jnp.int32, (BLOCK, 2 * BLOCK), 1), BLOCK)
    incl = jnp.where(t_id >= s_id, 1.0, 0.0).astype(BF16)
    low = lax.broadcasted_iota(jnp.int32, (BLOCK, LANES), 1) < breadth
    low_s = lax.broadcasted_iota(jnp.int32, (breadth, LANES), 1) < breadth
    head_i = lax.broadcasted_iota(jnp.int32, (LANES, LANES), 0) // breadth
    head_j = lax.broadcasted_iota(jnp.int32, (LANES, LANES), 1) // breadth
    ones = jnp.where(head_i == head_j, 1.0, 0.0).astype(BF16)
    means = jnp.where(head_i == head_j, 1.0 / breadth, 0.0).astype(BF16)

    for i in range(4):
        locals_[i].wait()
        remotes[i].wait_recv()

    def decays(q, c):
        lanes = pl.ds(pl.multiple_of(q * QUAD, QUAD), QUAD)
        states = [jnp.zeros((breadth, LANES), F32) for _ in range(2)]
        pref = jnp.zeros((1, QUAD), F32)
        for b in range(blocks):
            at = pl.ds(b * BLOCK, BLOCK)
            log_decay = -jnp.exp(fade[at, lanes].astype(F32))
            hi = log_decay.astype(BF16)
            lo = (log_decay - hi.astype(F32)).astype(BF16)
            cum = dot(incl, jnp.concatenate([hi, lo], axis=0))
            mid, total = cum[BLOCK // 2 - 1 : BLOCK // 2], cum[BLOCK - 1 :]
            km = (key[at, lanes].astype(F32) * jnp.exp(mid - cum)).astype(BF16)
            rec_mid[at, lanes] = (
                rec[at, lanes].astype(F32) * jnp.exp(cum - log_decay - mid)
            ).astype(BF16)
            key_mid[at, lanes] = km
            pref_row[b, :, lanes] = pref
            mid_row[b, :, lanes] = mid
            vb = val[at, lanes]
            end, whole = jnp.exp(total - mid), jnp.exp(total)
            for j in range(2):
                cut = slice(j * LANES, (j + 1) * LANES)
                entering[b, 2 * q + j] = states[j]
                product = dot_tn(vb[:, cut], km[:, cut])
                own = jnp.where(low_s, product[:breadth], product[breadth:])
                states[j] = states[j] * whole[:, cut] + own * end[:, cut]
            pref = pref + total
        for j in range(2):
            cut = slice(j * LANES, (j + 1) * LANES)
            for s in range(per_pair):
                slot = (2 * q + j) * per_pair + s
                outbox[slot] = states[j][s * piece : (s + 1) * piece].astype(BF16)
                outdec[slot] = pref[:, cut]
        return c

    lax.fori_loop(0, quads, decays, 0)

    inbox[me] = outbox[me]
    indec[me] = outdec[me]

    def state_copies(d):
        peer = lax.rem(me + d, n)
        return (
            pltpu.make_async_remote_copy(
                src_ref=outbox.at[peer], dst_ref=inbox.at[me],
                send_sem=s_send.at[d], recv_sem=s_recv.at[d],
                device_id=(peer, core), device_id_type=MESH,
            ),
            pltpu.make_async_remote_copy(
                src_ref=outdec.at[peer], dst_ref=indec.at[me],
                send_sem=d_send.at[d], recv_sem=d_recv.at[d],
                device_id=(peer, core), device_id_type=MESH,
            ),
        )

    def carry_copy(d):
        peer = lax.rem(me + d, n)
        return pltpu.make_async_remote_copy(
            src_ref=outbox2.at[peer], dst_ref=carry.at[me],
            send_sem=c_send.at[d], recv_sem=c_recv.at[d],
            device_id=(peer, core), device_id_type=MESH,
        )

    def send_states(d, c):
        for copy in state_copies(d):
            copy.start()
        return c

    lax.fori_loop(1, n, send_states, 0)

    def within(q, c):
        for j in range(2):
            lanes = pl.ds(pl.multiple_of(q * QUAD + j * LANES, LANES), LANES)
            reward = reward_ref[:, lanes]
            for b in range(blocks):
                at = pl.ds(b * BLOCK, BLOCK)
                vb = val[at, lanes]
                scores = dot_nt(rec_mid[at, lanes], split_heads(key_mid[at, lanes], low))
                scores = jnp.where(t_id > s_id, scores, 0.0).astype(BF16)
                own = rec[at, lanes].astype(F32) * key[at, lanes].astype(F32) * reward
                local_out[at, lanes] = dot(scores, split_heads(vb, low)) + dot(
                    own.astype(BF16), ones
                ) * vb.astype(F32)
        return c

    half = quads // 2
    lax.fori_loop(0, half, within, 0)

    def wait_states(d, c):
        for copy in state_copies(d):
            copy.wait()
        return c

    lax.fori_loop(1, n, wait_states, 0)

    def scan(i, run):
        outbox2[i] = run.astype(BF16)
        return run * jnp.exp(indec[i]) + inbox[i].astype(F32)

    lax.fori_loop(0, n, scan, jnp.zeros((piece, LANES), F32))
    carry[me] = outbox2[me]

    def send_carry(d, c):
        carry_copy(d).start()
        return c

    lax.fori_loop(1, n, send_carry, 0)
    lax.fori_loop(half, quads, within, 0)
    locals_[4].wait()
    remotes[4].wait_recv()

    def wait_carry(d, c):
        carry_copy(d).wait()
        return c

    lax.fori_loop(1, n, wait_carry, 0)

    def finish(q, c):
        for j in range(2):
            pair = 2 * q + j
            lanes = pl.ds(pl.multiple_of(q * QUAD + j * LANES, LANES), LANES)
            gain = gain_ref[:, lanes]
            came = jnp.concatenate(
                [carry[pair * per_pair + s].astype(F32) for s in range(per_pair)], axis=0
            )
            for b in range(blocks):
                at = pl.ds(b * BLOCK, BLOCK)
                state = entering[b, pair] + jnp.exp(pref_row[b, :, lanes]) * came
                state = (state * jnp.exp(mid_row[b, :, lanes])).astype(BF16)
                o = local_out[at, lanes] + dot_nt(rec_mid[at, lanes], split_heads(state, low_s))
                hi = o.astype(BF16)
                lo = (o - hi.astype(F32)).astype(BF16)
                centred = o - (dot(hi, means) + dot(lo, means))
                var = dot((centred * centred).astype(BF16), means)
                g = gate[at, lanes].astype(F32)
                normed = centred * lax.rsqrt(var + EPS) * gain
                gated[at, lanes] = (normed * (g / (1.0 + jnp.exp(-g)))).astype(BF16)
        return c

    lax.fori_loop(0, quads, finish, 0)

    def part_copy(c):
        return pltpu.make_async_remote_copy(
            src_ref=snd.at[c], dst_ref=rcv.at[c],
            send_sem=p_send.at[c], recv_sem=p_recv.at[c],
            device_id=(me, other), device_id_type=MESH,
        )

    def out_copy(c):
        return pltpu.make_async_copy(
            outv.at[c], out_hbm.at[:, pl.ds(pl.multiple_of(c * CHUNK, CHUNK), CHUNK)], o_sem.at[c]
        )

    def give(c, x):
        weight_copy(c).wait()
        snd[c] = dot(gated[their_rows, :], weight[c]).astype(BF16)
        part_copy(c).start()
        return x

    lax.fori_loop(0, chunks, give, 0)

    def take(c, x):
        mine = dot(gated[my_rows, :], weight[c])
        part_copy(c).wait_recv()
        outv[c] = (mine + rcv[c].astype(F32)).astype(BF16)
        out_copy(c).start()
        return x

    lax.fori_loop(0, chunks, take, 0)

    def drain(c, x):
        part_copy(c).wait_send()
        out_copy(c).wait()
        return x

    lax.fori_loop(0, chunks, drain, 0)
    for copy in remotes:
        copy.wait_send()


def shards(n, rec, key, val, fade, gate, reward, gain, mapping):
    rows = rec.shape[0]
    breadth = reward.shape[1]
    width = mapping.shape[0]
    depth = mapping.shape[1]
    tokens = rows * rec.shape[1] // width
    blocks, pairs, chunks = tokens // BLOCK, width // LANES, depth // CHUNK
    piece = pairs * breadth // n
    held = pltpu.VMEM((tokens, width), BF16)
    dma = pltpu.SemaphoreType.DMA
    anywhere = pl.BlockSpec(memory_space=pl.ANY)
    vmem = pl.BlockSpec(memory_space=pltpu.VMEM)
    return pl.pallas_call(
        functools.partial(kernel, n, breadth),
        out_shape=jax.ShapeDtypeStruct((rows, depth), BF16),
        in_specs=[anywhere] * 5 + [vmem] * 2 + [anywhere],
        out_specs=anywhere,
        scratch_shapes=[
            held, held, held, held, held,
            pltpu.VMEM((chunks, width, CHUNK), BF16),
            held, held,
            pltpu.VMEM((tokens, width), F32),
            pltpu.VMEM((blocks, pairs, breadth, LANES), F32),
            pltpu.VMEM((blocks, 1, width), F32),
            pltpu.VMEM((blocks, 1, width), F32),
            pltpu.VMEM((n, piece, LANES), BF16),
            pltpu.VMEM((n, 1, LANES), F32),
            pltpu.VMEM((n, piece, LANES), BF16),
            pltpu.VMEM((n, 1, LANES), F32),
            pltpu.VMEM((n, piece, LANES), BF16),
            pltpu.VMEM((n, piece, LANES), BF16),
            held,
            pltpu.VMEM((chunks, rows, CHUNK), BF16),
            pltpu.VMEM((chunks, rows, CHUNK), BF16),
            pltpu.VMEM((chunks, rows, CHUNK), BF16),
            dma((5,)), dma((5,)), dma((5,)), dma((chunks,)),
            dma((n,)), dma((n,)), dma((n,)), dma((n,)), dma((n,)), dma((n,)),
            dma((chunks,)), dma((chunks,)), dma((chunks,)),
        ],
        compiler_params=pltpu.CompilerParams(
            collective_id=0, has_side_effects=True, vmem_limit_bytes=56 * 2**20
        ),
    )(rec, key, val, fade, gate, reward.reshape(1, -1), gain.reshape(1, -1), mapping)


def solution(mesh):
    tokens = P(("seq", "head"), None)
    placed = (tokens,) * 5 + (P("head", None), P("head"), P("head", None))
    return jax.shard_map(
        functools.partial(shards, mesh.shape["seq"]),
        mesh=mesh, in_specs=placed, out_specs=tokens, check_vma=False,
    )
```
